32 devices in a mesh: north: 8 (over y, x, core), east: 4 (over z).
Axes of the slice: x: 2, y: 2, z: 4, core: 2. Of those that a mesh axis runs over, the one named last changes fastest.
Arguments:
- right_side: float32 [512, 256, 256], P('north', 'east'), may hold values from -6 to 6
- first_guess: float32 [512, 256, 256], P('north', 'east'), may hold values from -6 to 6
- mass_term: float32 [512, 256, 256], P('north', 'east'), may hold values from 0.1 to 0.9
Outputs:
- corrected: float32 [512, 256, 256], P('north', 'east')
- remaining: float32 [512, 256, 256], P('north', 'east')
The draws below stay inside these ranges and needn't reach their ends.
All inputs are finite; a program needn't handle non-finite values.
Results may differ from the reference program's by a relative error of at most 0.000032.
Values sent between devices are 32-bit elements; how exact they have to be, the bound alone decides.
A program may use at most 128 MiB of HBM per device.

```python
import jax
import jax.numpy as jnp
from jax import lax

CASES = 256
RATIO = 2
BEFORE = 2
AFTER = 2
INNER = 7
GRID_Y = 512
GRID_X = 256


def steps_of(key, dims, split, smallest, largest):
    loudness, own = 1.0, jax.random.fold_in(key, 6)
    for axis_at, shards_of in split:
        draws = jnp.exp(jax.random.uniform(jax.random.fold_in(own, axis_at), (shards_of,), jnp.float32, smallest / len(split), largest / len(split)))
        loudness = loudness * jnp.repeat(draws, dims[axis_at] // shards_of).reshape([-1 if axis == axis_at else 1 for axis in range(len(dims))])
    return loudness


def gaussian(stream_key, extent, width, bound, pieces=(), dtype=jnp.bfloat16):
    entries = width * jax.random.normal(stream_key, extent, jnp.float32)
    if pieces:
        entries = entries * steps_of(stream_key, extent, pieces, -0.22, 0.18)
    return jnp.clip(entries, -bound, bound).astype(dtype)


def setup_inputs(seed: int = 0) -> dict:
    key_of = jax.random.split(jax.random.key(seed), 4)
    right_side = gaussian(key_of[0], (GRID_Y, GRID_X, CASES), 1.0, 6.0, ((0, 8), (1, 4)), jnp.float32)
    first_guess = gaussian(key_of[1], (GRID_Y, GRID_X, CASES), 1.0, 6.0, ((0, 8), (1, 4)), jnp.float32)
    mass_term = jnp.clip(0.1 + 0.79999997 * jax.random.uniform(key_of[2], (GRID_Y, GRID_X, CASES), jnp.float32) ** steps_of(key_of[2], (GRID_Y, GRID_X, CASES), ((0, 8), (1, 4)), -0.2, 0.2), 0.1, 0.9)
    return dict(right_side=right_side, first_guess=first_guess, mass_term=mass_term)


def cross_sum(padded):
    inner_y, inner_x = padded.shape[0] - 2, padded.shape[1] - 2
    middle_rows = lax.slice_in_dim(padded, 1, 1 + inner_y, axis=0)
    middle_columns = lax.slice_in_dim(padded, 1, 1 + inner_x, axis=1)
    return (lax.slice_in_dim(middle_columns, 0, inner_y, axis=0) + lax.slice_in_dim(middle_columns, 2, 2 + inner_y, axis=0)
            + lax.slice_in_dim(middle_rows, 0, inner_x, axis=1) + lax.slice_in_dim(middle_rows, 2, 2 + inner_x, axis=1))


def smooth_step(padded, values, load, mass_here):
    return values + 0.8 * (load + cross_sum(padded) - (4.0 + mass_here) * values) / (4.0 + mass_here)


def block_means(values):
    cut = values.reshape(values.shape[0] // RATIO, RATIO, values.shape[1] // RATIO, RATIO, values.shape[2])
    return jnp.mean(cut, axis=(1, 3))


def spread_blocks(values):
    return jnp.repeat(jnp.repeat(values, RATIO, axis=0), RATIO, axis=1)


def reference(right_side, first_guess, mass_term):
    values = first_guess
    for sweep in range(BEFORE):
        values = smooth_step(jnp.pad(values, ((1, 1), (1, 1), (0, 0)), mode="wrap"), values, right_side, mass_term)
    defect = right_side + cross_sum(jnp.pad(values, ((1, 1), (1, 1), (0, 0)), mode="wrap")) - (4.0 + mass_term) * values
    coarse_load, coarse_mass = block_means(defect) * RATIO, block_means(mass_term) * RATIO
    coarse_values = jnp.zeros_like(coarse_load)
    for sweep in range(INNER):
        coarse_values = smooth_step(jnp.pad(coarse_values, ((1, 1), (1, 1), (0, 0)), mode="wrap"), coarse_values, coarse_load, coarse_mass)
    values = values + spread_blocks(coarse_values)
    for sweep in range(AFTER):
        values = smooth_step(jnp.pad(values, ((1, 1), (1, 1), (0, 0)), mode="wrap"), values, right_side, mass_term)
    corrected = values
    remaining = right_side + cross_sum(jnp.pad(corrected, ((1, 1), (1, 1), (0, 0)), mode="wrap")) - (4.0 + mass_term) * corrected
    return corrected, remaining
```

```python
import functools

import jax
import jax.numpy as jnp
from jax import lax
from jax.experimental import pallas as pl
from jax.experimental.pallas import tpu as pltpu
from jax.sharding import PartitionSpec as P

RATIO = 2
INNER = 7
AXES = ("north", "east")
MESH = pl.DeviceIdType.MESH


def ring(axis):
    count, me = lax.axis_size(axis), lax.axis_index(axis)
    return lax.rem(me + count - 1, count), lax.rem(me + 1, count)


def place(axis, index):
    return tuple(index if name == axis else lax.axis_index(name) for name in AXES)


class Level:
    def __init__(self, rows, cols, grids, sent, got, send_sem, recv_sem):
        self.rows, self.cols = rows, cols
        self.grids, self.sent, self.got = grids, sent, got
        self.send_sem, self.recv_sem = send_sem, recv_sem

    def copies(self, p):
        grid = self.grids[p]
        north_low, north_high = ring("north")
        east_low, east_high = ring("east")
        moves = (
            (grid.at[1], grid.at[self.rows + 1], place("north", north_low)),
            (grid.at[self.rows], grid.at[0], place("north", north_high)),
            (self.sent.at[p, 0], self.got.at[p, 1], place("east", east_low)),
            (self.sent.at[p, 1], self.got.at[p, 0], place("east", east_high)),
        )
        return [
            pltpu.make_async_remote_copy(
                src_ref=source,
                dst_ref=target,
                send_sem=self.send_sem.at[p, k],
                recv_sem=self.recv_sem.at[p, k],
                device_id=device,
                device_id_type=MESH,
            )
            for k, (source, target, device) in enumerate(moves)
        ]

    def start(self, p):
        for copy in self.copies(p):
            copy.start()

    def wait(self, p):
        for copy in self.copies(p):
            copy.wait()

    def around(self, p, y, x0, x1):
        grid = self.grids[p]
        a0, a1 = max(x0 - 8, 0), min(x1 + 8, self.cols)
        wide = grid[y, a0:a1, :]
        count = a1 - a0
        low = pltpu.roll(wide, 1, 0)[x0 - a0 : x1 - a0]
        high = pltpu.roll(wide, count - 1, 0)[x0 - a0 : x1 - a0]
        where = lax.broadcasted_iota(jnp.int32, (8, wide.shape[1]), 0)
        if x0 == 0:
            first = jnp.where(where == 0, self.got[p, 0, pl.ds(y - 1, 1), :], low[:8])
            low = first if x1 == 8 else jnp.concatenate([first, low[8:]], axis=0)
        if x1 == self.cols:
            last = jnp.where(where == 7, self.got[p, 1, pl.ds(y - 1, 1), :], high[-8:])
            high = last if x1 - x0 == 8 else jnp.concatenate([high[:-8], last], axis=0)
        total = (low + high) + (grid[y - 1, x0:x1, :] + grid[y + 1, x0:x1, :])
        return wide[x0 - a0 : x1 - a0], total

    def inside(self, cell):
        if self.cols > 16:

            def row(y, carry):
                cell(y, 8, self.cols - 8)
                return carry

            lax.fori_loop(2, self.rows, row, 0, unroll=2)

    def rim(self, cell):
        def row(y, carry):
            cell(y, 0, 8)
            cell(y, self.cols - 8, self.cols)
            return carry

        lax.fori_loop(1, self.rows + 1, row, 0, unroll=4)
        if self.cols > 16:
            cell(1, 8, self.cols - 8)
            cell(self.rows, 8, self.cols - 8)

    def put(self, p, y, x0, x1, new):
        self.grids[p][y, x0:x1, :] = new
        if x0 == 0:
            self.sent[p, 0, pl.ds(y - 1, 1), :] = new[:1]
        if x1 == self.cols:
            self.sent[p, 1, pl.ds(y - 1, 1), :] = new[-1:]

    def sweep(self, p, load, scale):
        def cell(y, x0, x1):
            here, total = self.around(p, y, x0, x1)
            new = 0.2 * here + scale[y - 1, x0:x1, :] * (load[y - 1, x0:x1, :] + total)
            self.put(1 - p, y, x0, x1, new)

        self.start(p)
        self.inside(cell)
        self.wait(p)
        self.rim(cell)


def kernel(
    load_hbm, guess_hbm, mass_hbm, fixed_hbm, left_hbm,
    load, mass, scale, fine_a, fine_b, fine_sent, fine_got,
    thick, cload, cscale, coarse_a, coarse_b, coarse_sent, coarse_got, spread,
    fine_send, fine_recv, coarse_send, coarse_recv, local,
):
    rows, cols, cases = load.shape
    half_rows, half_cols = rows // RATIO, cols // RATIO
    parts = cases // 128
    fine = Level(rows, cols, (fine_a, fine_b), fine_sent, fine_got, fine_send, fine_recv)
    coarse = Level(
        half_rows, half_cols, (coarse_a, coarse_b),
        coarse_sent, coarse_got, coarse_send, coarse_recv,
    )
    fetch_guess = pltpu.make_async_copy(guess_hbm, fine_a.at[pl.ds(1, rows)], local.at[0])
    fetch_mass = pltpu.make_async_copy(mass_hbm, mass, local.at[1])
    fetch_load = pltpu.make_async_copy(load_hbm, load, local.at[2])
    fetch_guess.start()
    fetch_mass.start()
    fetch_load.start()

    barrier = pltpu.get_barrier_semaphore()
    for axis in AXES:
        for other in ring(axis):
            pl.semaphore_signal(barrier, inc=1, device_id=place(axis, other), device_id_type=MESH)
    pl.semaphore_wait(barrier, 4)

    fetch_guess.wait()

    def pack(y, carry):
        fine_sent[0, 0, pl.ds(y, 1), :] = fine_a[y + 1, 0:8, :][:1]
        fine_sent[0, 1, pl.ds(y, 1), :] = fine_a[y + 1, cols - 8 : cols, :][-1:]
        return carry

    lax.fori_loop(0, rows, pack, 0, unroll=4)
    fetch_mass.wait()
    fetch_load.wait()

    def first(y, x0, x1):
        here, total = fine.around(0, y, x0, x1)
        weight = 0.8 / (4.0 + mass[y - 1, x0:x1, :])
        scale[y - 1, x0:x1, :] = weight
        fine.put(1, y, x0, x1, 0.2 * here + weight * (load[y - 1, x0:x1, :] + total))

    fine.start(0)
    fine.inside(first)
    fine.wait(0)
    fine.rim(first)
    fine.sweep(1, load, scale)

    def defect(y, x0, x1):
        here, total = fine.around(0, y, x0, x1)
        return load[y - 1, x0:x1, :] + total - (4.0 + mass[y - 1, x0:x1, :]) * here

    fine.start(0)
    fine.wait(0)

    def gather(y, carry):
        sums = (
            defect(2 * y + 1, 0, cols) + defect(2 * y + 2, 0, cols),
            mass[2 * y] + mass[2 * y + 1],
        )
        for k in range(2):
            for h in range(parts):
                thick[k, h] = sums[k][:, h * 128 : (h + 1) * 128]
        pair = [
            jnp.concatenate(
                [
                    thick.at[k, h][pl.ds(0, half_cols, stride=2), :]
                    + thick.at[k, h][pl.ds(1, half_cols, stride=2), :]
                    for h in range(parts)
                ],
                axis=1,
            )
            for k in range(2)
        ]
        new_load = 0.5 * pair[0]
        weight = 0.8 / (4.0 + 0.5 * pair[1])
        cload[y] = new_load
        cscale[y] = weight
        coarse.put(0, y + 1, 0, half_cols, weight * new_load)
        return carry

    lax.fori_loop(0, half_rows, gather, 0)

    for sweep in range(INNER - 1):
        coarse.sweep(sweep % 2, cload, cscale)
    coarse_last = (coarse_a, coarse_b)[(INNER - 1) % 2]

    def correct(y, carry):
        value = coarse_last[y + 1]
        for h in range(parts):
            part = value[:, h * 128 : (h + 1) * 128]
            spread.at[h][pl.ds(0, half_cols, stride=2), :] = part
            spread.at[h][pl.ds(1, half_cols, stride=2), :] = part
        added = jnp.concatenate([spread[h] for h in range(parts)], axis=1)
        for k in range(2):
            at = 2 * y + 1 + k
            fine.put(1, at, 0, cols, fine_a[at] + added)
        return carry

    lax.fori_loop(0, half_rows, correct, 0)
    fine.sweep(1, load, scale)
    fine.sweep(0, load, scale)

    give_fixed = pltpu.make_async_copy(fine_b.at[pl.ds(1, rows)], fixed_hbm, local.at[0])
    fine.start(1)
    give_fixed.start()

    def left(y, x0, x1):
        here, total = fine.around(1, y, x0, x1)
        scale[y - 1, x0:x1, :] = (
            load[y - 1, x0:x1, :] + total - (4.0 + mass[y - 1, x0:x1, :]) * here
        )

    fine.inside(left)
    fine.wait(1)
    fine.rim(left)
    give_left = pltpu.make_async_copy(scale, left_hbm, local.at[1])
    give_left.start()
    give_fixed.wait()
    give_left.wait()


def body(right_side, first_guess, mass_term):
    rows, cols, cases = right_side.shape
    half_rows, half_cols = rows // RATIO, cols // RATIO
    whole = jax.ShapeDtypeStruct(right_side.shape, jnp.float32)
    any_space = pl.BlockSpec(memory_space=pl.ANY)

    def vmem(*shape):
        return pltpu.VMEM(shape, jnp.float32)

    return pl.pallas_call(
        kernel,
        out_shape=(whole, whole),
        in_specs=[any_space] * 3,
        out_specs=(any_space, any_space),
        scratch_shapes=[
            vmem(rows, cols, cases),
            vmem(rows, cols, cases),
            vmem(rows, cols, cases),
            vmem(rows + 2, cols, cases),
            vmem(rows + 2, cols, cases),
            vmem(2, 2, rows, cases),
            vmem(2, 2, rows, cases),
            vmem(2, cases // 128, cols, 128),
            vmem(half_rows, half_cols, cases),
            vmem(half_rows, half_cols, cases),
            vmem(half_rows + 2, half_cols, cases),
            vmem(half_rows + 2, half_cols, cases),
            vmem(2, 2, half_rows, cases),
            vmem(2, 2, half_rows, cases),
            vmem(cases // 128, cols, 128),
            pltpu.SemaphoreType.DMA((2, 4)),
            pltpu.SemaphoreType.DMA((2, 4)),
            pltpu.SemaphoreType.DMA((2, 4)),
            pltpu.SemaphoreType.DMA((2, 4)),
            pltpu.SemaphoreType.DMA((3,)),
        ],
        compiler_params=pltpu.CompilerParams(
            collective_id=0, has_side_effects=True, vmem_limit_bytes=60 * 1024 * 1024
        ),
    )(right_side, first_guess, mass_term)


def solution(mesh):
    spec = P("north", "east", None)
    return jax.shard_map(
        body, mesh=mesh, in_specs=(spec, spec, spec), out_specs=(spec, spec), check_vma=False
    )
```

```python
import functools

import jax
import jax.numpy as jnp
from jax import lax
from jax.experimental import pallas as pl
from jax.experimental.pallas import tpu as pltpu
from jax.sharding import PartitionSpec as P

RATIO = 2
INNER = 7
NEAR = (INNER - 1) // 2
DEPTH = INNER - NEAR
SCALE_AT = 1
AXES = ("north", "east")
MESH = pl.DeviceIdType.MESH


def ring(axis):
    count, me = lax.axis_size(axis), lax.axis_index(axis)
    return lax.rem(me + count - 1, count), lax.rem(me + 1, count)


def place(axis, index):
    return tuple(index if name == axis else lax.axis_index(name) for name in AXES)


class Level:
    def __init__(self, rows, cols, grids, sent, got, send_sem, recv_sem):
        self.rows, self.cols = rows, cols
        self.grids, self.sent, self.got = grids, sent, got
        self.send_sem, self.recv_sem = send_sem, recv_sem

    def copies(self, p):
        grid = self.grids[p]
        north_low, north_high = ring("north")
        east_low, east_high = ring("east")
        moves = (
            (grid.at[1], grid.at[self.rows + 1], place("north", north_low)),
            (grid.at[self.rows], grid.at[0], place("north", north_high)),
            (self.sent.at[p, 0], self.got.at[p, 1], place("east", east_low)),
            (self.sent.at[p, 1], self.got.at[p, 0], place("east", east_high)),
        )
        return [
            pltpu.make_async_remote_copy(
                src_ref=source,
                dst_ref=target,
                send_sem=self.send_sem.at[p, k],
                recv_sem=self.recv_sem.at[p, k],
                device_id=device,
                device_id_type=MESH,
            )
            for k, (source, target, device) in enumerate(moves)
        ]

    def start(self, p):
        for copy in self.copies(p):
            copy.start()

    def wait(self, p):
        for copy in self.copies(p):
            copy.wait()

    def around(self, p, y, x0, x1, outer=True):
        grid = self.grids[p]
        a0, a1 = max(x0 - 8, 0), min(x1 + 8, self.cols)
        wide = grid[y, a0:a1, :]
        count = a1 - a0
        low = pltpu.roll(wide, 1, 0)[x0 - a0 : x1 - a0]
        high = pltpu.roll(wide, count - 1, 0)[x0 - a0 : x1 - a0]
        where = lax.broadcasted_iota(jnp.int32, (8, wide.shape[1]), 0)
        if x0 == 0:
            first = jnp.where(
                where == 0, self.got[p, 0, pl.ds(y - 1, 1), :] if outer else 0.0, low[:8]
            )
            low = first if x1 == 8 else jnp.concatenate([first, low[8:]], axis=0)
        if x1 == self.cols:
            last = jnp.where(
                where == 7, self.got[p, 1, pl.ds(y - 1, 1), :] if outer else 0.0, high[-8:]
            )
            high = last if x1 - x0 == 8 else jnp.concatenate([high[:-8], last], axis=0)
        total = (low + high) + (grid[y - 1, x0:x1, :] + grid[y + 1, x0:x1, :])
        return wide[x0 - a0 : x1 - a0], total

    def inside(self, cell):
        if self.cols > 16:

            def row(y, carry):
                cell(y, 8, self.cols - 8)
                return carry

            lax.fori_loop(2, self.rows, row, 0, unroll=2)

    def rim(self, cell):
        def row(y, carry):
            cell(y, 0, 8)
            cell(y, self.cols - 8, self.cols)
            return carry

        lax.fori_loop(1, self.rows + 1, row, 0, unroll=4)
        if self.cols > 16:
            cell(1, 8, self.cols - 8)
            cell(self.rows, 8, self.cols - 8)

    def put(self, p, y, x0, x1, new):
        self.grids[p][y, x0:x1, :] = new
        if x0 == 0:
            self.sent[p, 0, pl.ds(y - 1, 1), :] = new[:1]
        if x1 == self.cols:
            self.sent[p, 1, pl.ds(y - 1, 1), :] = new[-1:]

    def sweep(self, p, load, scale, begun=False, own=False):
        def cell(y, x0, x1):
            here, total = self.around(p, y, x0, x1)
            new = 0.2 * here + scale[y - 1, x0:x1, :] * (load[y - 1, x0:x1, :] + total)
            self.put(1 - p, y, x0, x1, new)

        if own:

            def row(y, carry):
                cell(y, 0, self.cols)
                return carry

            lax.fori_loop(1, self.rows + 1, row, 0, unroll=2)
            return
        if not begun:
            self.start(p)
        self.inside(cell)
        self.wait(p)
        self.rim(cell)


def offsets(size, depth, pad, side):
    if side < 0:
        return pad, pad + size, depth
    if side > 0:
        return pad + size - depth, pad - depth, depth
    return pad, pad, size


def deep_copies(wide, depth, size, sends, recvs):
    sides = {axis: (ring(axis)[0], lax.axis_index(axis), ring(axis)[1]) for axis in AXES}
    copies = []
    for dy in (-1, 0, 1):
        for dx in (-1, 0, 1):
            if dy == 0 and dx == 0:
                continue
            from_y, to_y, high = offsets(size[0], depth, DEPTH, dy)
            from_x, to_x, across = offsets(size[1], depth, 8, dx)
            copies.append(
                pltpu.make_async_remote_copy(
                    src_ref=wide.at[pl.ds(from_y, high), pl.ds(from_x, across)],
                    dst_ref=wide.at[pl.ds(to_y, high), pl.ds(to_x, across)],
                    send_sem=sends.at[len(copies)],
                    recv_sem=recvs.at[len(copies)],
                    device_id=(sides["north"][dy + 1], sides["east"][dx + 1]),
                    device_id_type=MESH,
                )
            )
    return copies


def kernel(
    load_hbm, guess_hbm, mass_hbm, fixed, left_out,
    load, mass, scale, fine_a, fine_b, fine_sent, fine_got,
    thick, cload, cscale, coarse_a, coarse_b, coarse_c, spread,
    fine_send, fine_recv, coarse_send, coarse_recv, local,
):
    rows, cols, cases = load.shape
    half_rows, half_cols = rows // RATIO, cols // RATIO
    parts = cases // 128
    fine = Level(rows, cols, (fine_a, fine_b), fine_sent, fine_got, fine_send, fine_recv)
    fetch_guess = pltpu.make_async_copy(guess_hbm, fine_a.at[pl.ds(1, rows)], local.at[0])
    fetch_mass = pltpu.make_async_copy(mass_hbm, mass, local.at[1])
    fetch_load = pltpu.make_async_copy(load_hbm, load, local.at[2])
    fetch_guess.start()
    fetch_mass.start()
    fetch_load.start()

    barrier = pltpu.get_barrier_semaphore()
    norths = (ring("north")[0], lax.axis_index("north"), ring("north")[1])
    easts = (ring("east")[0], lax.axis_index("east"), ring("east")[1])
    for dy in range(3):
        for dx in range(3):
            if (dy, dx) != (1, 1):
                pl.semaphore_signal(
                    barrier, inc=1, device_id=(norths[dy], easts[dx]), device_id_type=MESH
                )
    pl.semaphore_wait(barrier, 8)

    fetch_guess.wait()

    def pack(y, carry):
        fine_sent[0, 0, pl.ds(y, 1), :] = fine_a[y + 1, 0:8, :][:1]
        fine_sent[0, 1, pl.ds(y, 1), :] = fine_a[y + 1, cols - 8 : cols, :][-1:]
        return carry

    lax.fori_loop(0, rows, pack, 0, unroll=4)
    fine.start(0)

    def pairs(k, total):
        for h in range(parts):
            thick[k, h] = total[:, h * 128 : (h + 1) * 128]
        return jnp.concatenate(
            [
                thick.at[k, h][pl.ds(0, half_cols, stride=2), :]
                + thick.at[k, h][pl.ds(1, half_cols, stride=2), :]
                for h in range(parts)
            ],
            axis=1,
        )

    fetch_mass.wait()

    def gather_mass(y, carry):
        total = pairs(0, mass[2 * y] + mass[2 * y + 1])
        cscale[y + DEPTH, 8 : 8 + half_cols, :] = 0.8 / (4.0 + 0.5 * total)
        return carry

    lax.fori_loop(0, half_rows, gather_mass, 0, unroll=2)
    size = (half_rows, half_cols)
    send_scale = deep_copies(cscale, NEAR, size, coarse_send.at[0], coarse_recv.at[0])
    send_load = deep_copies(cload, NEAR, size, coarse_send.at[1], coarse_recv.at[1])
    send_value = deep_copies(coarse_c, DEPTH, size, coarse_send.at[2], coarse_recv.at[2])
    if SCALE_AT == 0:
        for copy in send_scale:
            copy.start()
    fetch_load.wait()

    def first(y, x0, x1):
        here, total = fine.around(0, y, x0, x1)
        weight = 0.8 / (4.0 + mass[y - 1, x0:x1, :])
        scale[y - 1, x0:x1, :] = weight
        fine.put(1, y, x0, x1, 0.2 * here + weight * (load[y - 1, x0:x1, :] + total))

    fine.inside(first)
    fine.wait(0)
    fine.rim(first)
    if SCALE_AT == 1:
        fine.start(1)
        for copy in send_scale:
            copy.start()
        fine.sweep(1, load, scale, begun=True)
    else:
        fine.sweep(1, load, scale)

    def defect(y, outer):
        here, total = fine.around(0, y, 0, cols, outer)
        return load[y - 1] + total - (4.0 + mass[y - 1]) * here

    def gather(y, outer):
        total = pairs(y % 2, defect(2 * y + 1, outer) + defect(2 * y + 2, outer))
        cload[y + DEPTH, 8 : 8 + half_cols, :] = 0.5 * total

    def gather_inner(y, carry):
        gather(y, False)
        return carry

    def gather_outer(y, carry):
        where = lax.broadcasted_iota(jnp.int32, (8, cases), 0)
        low = fine_got[0, 0, pl.ds(2 * y, 1), :] + fine_got[0, 0, pl.ds(2 * y + 1, 1), :]
        high = fine_got[0, 1, pl.ds(2 * y, 1), :] + fine_got[0, 1, pl.ds(2 * y + 1, 1), :]
        cload[y + DEPTH, 8:16, :] += jnp.where(where == 0, 0.5 * low, 0.0)
        cload[y + DEPTH, half_cols : half_cols + 8, :] += jnp.where(where == 7, 0.5 * high, 0.0)
        return carry

    fine.start(0)
    if SCALE_AT == 2:
        for copy in send_scale:
            copy.start()
    lax.fori_loop(1, half_rows - 1, gather_inner, 0, unroll=2)
    fine.wait(0)
    lax.fori_loop(1, half_rows - 1, gather_outer, 0, unroll=2)
    gather(0, True)
    gather(half_rows - 1, True)
    for end in (0, rows + 1):
        fine_b[end] = fine_a[end]
    for side in range(2):
        fine_got[1, side] = fine_got[0, side]
    for copy in send_load:
        copy.start()
    for copy in send_scale:
        copy.wait()
    for copy in send_load:
        copy.wait()

    tall, broad = cload.shape[0], cload.shape[1]

    def begin(y, carry):
        coarse_a[y] = cscale[y] * cload[y]
        return carry

    margin = DEPTH - NEAR
    lax.fori_loop(margin, tall - margin, begin, 0, unroll=2)

    def sweeps(chain, margin):
        for step, (old, new) in enumerate(zip(chain, chain[1:]), 1):
            own = new is coarse_c

            def row(y, carry, old=old, new=new, own=own):
                here = old[y]
                total = (pltpu.roll(here, 1, 0) + pltpu.roll(here, broad - 1, 0)) + (
                    old[y - 1] + old[y + 1]
                )
                value = 0.2 * here + cscale[y] * (cload[y] + total)
                if own:
                    new[y, 8 : 8 + half_cols, :] = value[8 : 8 + half_cols]
                else:
                    new[y] = value
                return carry

            lax.fori_loop(margin + step, tall - margin - step, row, 0, unroll=2)

    grids = (coarse_a, coarse_b)
    sweeps([grids[step % 2] for step in range(NEAR)] + [coarse_c], margin)
    for copy in send_value:
        copy.start()
    for copy in send_value:
        copy.wait()
    rest = INNER - 1 - NEAR
    sweeps([coarse_c] + [grids[step % 2] for step in range(rest)], 0)
    last = grids[(rest - 1) % 2]

    def widen(k, y):
        for h in range(parts):
            part = last[y, 8 : 8 + half_cols, h * 128 : (h + 1) * 128]
            spread.at[k, h][pl.ds(0, half_cols, stride=2), :] = part
            spread.at[k, h][pl.ds(1, half_cols, stride=2), :] = part
        return jnp.concatenate([spread[k, h] for h in range(parts)], axis=1)

    def correct(y, carry):
        added = widen(y % 2, y + DEPTH)
        low = last[y + DEPTH, 0:8, :][-1:]
        high = last[y + DEPTH, 8 + half_cols : 16 + half_cols, :][:1]
        for k in range(2):
            at = 2 * y + 1 + k
            fine_b[at] = fine_a[at] + added
            fine_got[1, 0, pl.ds(at - 1, 1), :] += low
            fine_got[1, 1, pl.ds(at - 1, 1), :] += high
        return carry

    lax.fori_loop(0, half_rows, correct, 0, unroll=2)
    fine_b[0] += widen(0, DEPTH - 1)
    fine_b[rows + 1] += widen(1, DEPTH + half_rows)
    fine.sweep(1, load, scale, own=True)
    fine.sweep(0, load, scale)

    def left(y, x0, x1):
        here, total = fine.around(1, y, x0, x1)
        fixed[y - 1, x0:x1, :] = here
        left_out[y - 1, x0:x1, :] = (
            load[y - 1, x0:x1, :] + total - (4.0 + mass[y - 1, x0:x1, :]) * here
        )

    fine.start(1)
    fine.inside(left)
    fine.wait(1)
    fine.rim(left)


def body(right_side, first_guess, mass_term):
    rows, cols, cases = right_side.shape
    half_rows, half_cols = rows // RATIO, cols // RATIO
    whole = jax.ShapeDtypeStruct(right_side.shape, jnp.float32)
    any_space = pl.BlockSpec(memory_space=pl.ANY)

    def vmem(*shape):
        return pltpu.VMEM(shape, jnp.float32)

    fixed, left = pl.pallas_call(
        kernel,
        out_shape=(pltpu.VMEM(right_side.shape, jnp.float32), pltpu.VMEM(right_side.shape, jnp.float32)),
        in_specs=[any_space] * 3,
        out_specs=(pl.BlockSpec(memory_space=pltpu.VMEM),)*2,
        scratch_shapes=[
            vmem(rows, cols, cases),
            vmem(rows, cols, cases),
            vmem(rows, cols, cases),
            vmem(rows + 2, cols, cases),
            vmem(rows + 2, cols, cases),
            vmem(2, 2, rows, cases),
            vmem(2, 2, rows, cases),
            vmem(2, cases // 128, cols, 128),
            vmem(half_rows + 2 * DEPTH, half_cols + 16, cases),
            vmem(half_rows + 2 * DEPTH, half_cols + 16, cases),
            vmem(half_rows + 2 * DEPTH, half_cols + 16, cases),
            vmem(half_rows + 2 * DEPTH, half_cols + 16, cases),
            vmem(half_rows + 2 * DEPTH, half_cols + 16, cases),
            vmem(2, cases // 128, cols, 128),
            pltpu.SemaphoreType.DMA((2, 4)),
            pltpu.SemaphoreType.DMA((2, 4)),
            pltpu.SemaphoreType.DMA((3, 8)),
            pltpu.SemaphoreType.DMA((3, 8)),
            pltpu.SemaphoreType.DMA((3,)),
        ],
        compiler_params=pltpu.CompilerParams(
            collective_id=0, has_side_effects=True, vmem_limit_bytes=48 * 1024 * 1024
        ),
    )(right_side, first_guess, mass_term)
    return fixed, left


def solution(mesh):
    spec = P("north", "east", None)
    return jax.shard_map(
        body, mesh=mesh, in_specs=(spec, spec, spec), out_specs=(spec, spec), check_vma=False
    )
```

```python
import functools

import jax
import jax.numpy as jnp
from jax import lax
from jax.experimental import pallas as pl
from jax.experimental.pallas import tpu as pltpu
from jax.sharding import PartitionSpec as P

RATIO = 2
INNER = 7
NEAR = (INNER - 1) // 2
DEPTH = INNER - NEAR
SCALE_AT = 0
AXES = ("north", "east")
MESH = pl.DeviceIdType.MESH


def ring(axis):
    count, me = lax.axis_size(axis), lax.axis_index(axis)
    return lax.rem(me + count - 1, count), lax.rem(me + 1, count)


def place(axis, index):
    return tuple(index if name == axis else lax.axis_index(name) for name in AXES)


class Level:
    def __init__(self, rows, cols, grids, sent, got, send_sem, recv_sem):
        self.rows, self.cols = rows, cols
        self.grids, self.sent, self.got = grids, sent, got
        self.send_sem, self.recv_sem = send_sem, recv_sem

    def copies(self, p):
        grid = self.grids[p]
        north_low, north_high = ring("north")
        east_low, east_high = ring("east")
        moves = (
            (grid.at[1], grid.at[self.rows + 1], place("north", north_low)),
            (grid.at[self.rows], grid.at[0], place("north", north_high)),
            (self.sent.at[p, 0], self.got.at[p, 1], place("east", east_low)),
            (self.sent.at[p, 1], self.got.at[p, 0], place("east", east_high)),
        )
        return [
            pltpu.make_async_remote_copy(
                src_ref=source,
                dst_ref=target,
                send_sem=self.send_sem.at[p, k],
                recv_sem=self.recv_sem.at[p, k],
                device_id=device,
                device_id_type=MESH,
            )
            for k, (source, target, device) in enumerate(moves)
        ]

    def start(self, p):
        for copy in self.copies(p):
            copy.start()

    def wait(self, p):
        for copy in self.copies(p):
            copy.wait()

    def around(self, p, y, x0, x1, outer=True):
        grid = self.grids[p]
        a0, a1 = max(x0 - 8, 0), min(x1 + 8, self.cols)
        wide = grid[y, a0:a1, :]
        count = a1 - a0
        low = pltpu.roll(wide, 1, 0)[x0 - a0 : x1 - a0]
        high = pltpu.roll(wide, count - 1, 0)[x0 - a0 : x1 - a0]
        where = lax.broadcasted_iota(jnp.int32, (8, wide.shape[1]), 0)
        if x0 == 0:
            first = jnp.where(
                where == 0, self.got[p, 0, pl.ds(y - 1, 1), :] if outer else 0.0, low[:8]
            )
            low = first if x1 == 8 else jnp.concatenate([first, low[8:]], axis=0)
        if x1 == self.cols:
            last = jnp.where(
                where == 7, self.got[p, 1, pl.ds(y - 1, 1), :] if outer else 0.0, high[-8:]
            )
            high = last if x1 - x0 == 8 else jnp.concatenate([high[:-8], last], axis=0)
        total = (low + high) + (grid[y - 1, x0:x1, :] + grid[y + 1, x0:x1, :])
        return wide[x0 - a0 : x1 - a0], total

    def inside(self, cell):
        def row(y, carry):
            cell(y, 0, self.cols, False)
            return carry

        lax.fori_loop(2, self.rows, row, 0, unroll=2)

    def rim(self, p, cell, mend):
        def row(y, carry):
            low = self.got[p, 0, pl.ds(y - 1, 1), :]
            high = self.got[p, 1, pl.ds(y - 1, 1), :]
            where = lax.broadcasted_iota(jnp.int32, (8, low.shape[1]), 0)
            mend(y, 0, 8, jnp.where(where == 0, low, 0.0))
            mend(y, self.cols - 8, self.cols, jnp.where(where == 7, high, 0.0))
            return carry

        lax.fori_loop(2, self.rows, row, 0, unroll=4)
        cell(1, 0, self.cols)
        cell(self.rows, 0, self.cols)

    def put(self, p, y, x0, x1, new, outer=True):
        self.grids[p][y, x0:x1, :] = new
        if outer and x0 == 0:
            self.sent[p, 0, pl.ds(y - 1, 1), :] = new[:1]
        if outer and x1 == self.cols:
            self.sent[p, 1, pl.ds(y - 1, 1), :] = new[-1:]

    def mend(self, p, scale):
        def add(y, x0, x1, more):
            old = self.grids[1 - p][y, x0:x1, :]
            self.put(1 - p, y, x0, x1, old + scale[y - 1, x0:x1, :] * more)

        return add

    def sweep(self, p, load, scale, begun=False, own=False):
        def cell(y, x0, x1, outer=True):
            here, total = self.around(p, y, x0, x1, outer)
            new = 0.2 * here + scale[y - 1, x0:x1, :] * (load[y - 1, x0:x1, :] + total)
            self.put(1 - p, y, x0, x1, new, outer)

        if own:

            def row(y, carry):
                cell(y, 0, self.cols)
                return carry

            lax.fori_loop(1, self.rows + 1, row, 0, unroll=2)
            return
        if not begun:
            self.start(p)
        self.inside(cell)
        self.wait(p)
        self.rim(p, cell, self.mend(p, scale))


def offsets(size, depth, pad, side):
    if side < 0:
        return pad, pad + size, depth
    if side > 0:
        return pad + size - depth, pad - depth, depth
    return pad, pad, size


def deep_copies(wide, depth, size, sends, recvs):
    sides = {axis: (ring(axis)[0], lax.axis_index(axis), ring(axis)[1]) for axis in AXES}
    copies = []
    for dy in (-1, 0, 1):
        for dx in (-1, 0, 1):
            if dy == 0 and dx == 0:
                continue
            from_y, to_y, high = offsets(size[0], depth, DEPTH, dy)
            from_x, to_x, across = offsets(size[1], depth, 8, dx)
            copies.append(
                pltpu.make_async_remote_copy(
                    src_ref=wide.at[pl.ds(from_y, high), pl.ds(from_x, across)],
                    dst_ref=wide.at[pl.ds(to_y, high), pl.ds(to_x, across)],
                    send_sem=sends.at[len(copies)],
                    recv_sem=recvs.at[len(copies)],
                    device_id=(sides["north"][dy + 1], sides["east"][dx + 1]),
                    device_id_type=MESH,
                )
            )
    return copies


def kernel(
    load_hbm, guess_hbm, mass_hbm, fixed, left_out,
    load, mass, scale, fine_a, fine_b, fine_sent, fine_got,
    thick, cload, cscale, coarse_a, coarse_b, coarse_c, spread,
    fine_send, fine_recv, coarse_send, coarse_recv, local,
):
    rows, cols, cases = load.shape
    half_rows, half_cols = rows // RATIO, cols // RATIO
    parts = cases // 128
    fine = Level(rows, cols, (fine_a, fine_b), fine_sent, fine_got, fine_send, fine_recv)
    fetch_guess = pltpu.make_async_copy(guess_hbm, fine_a.at[pl.ds(1, rows)], local.at[0])
    fetch_mass = pltpu.make_async_copy(mass_hbm, mass, local.at[1])
    fetch_load = pltpu.make_async_copy(load_hbm, load, local.at[2])
    fetch_guess.start()

    barrier = pltpu.get_barrier_semaphore()
    norths = (ring("north")[0], lax.axis_index("north"), ring("north")[1])
    easts = (ring("east")[0], lax.axis_index("east"), ring("east")[1])
    for dy in range(3):
        for dx in range(3):
            if (dy, dx) != (1, 1):
                pl.semaphore_signal(
                    barrier, inc=1, device_id=(norths[dy], easts[dx]), device_id_type=MESH
                )
    pl.semaphore_wait(barrier, 8)

    fetch_guess.wait()
    fetch_mass.start()
    fetch_load.start()

    def pack(y, carry):
        fine_sent[0, 0, pl.ds(y, 1), :] = fine_a[y + 1, 0:8, :][:1]
        fine_sent[0, 1, pl.ds(y, 1), :] = fine_a[y + 1, cols - 8 : cols, :][-1:]
        return carry

    lax.fori_loop(0, rows, pack, 0, unroll=4)
    fine.start(0)

    def pairs(k, total):
        for h in range(parts):
            thick[k, h] = total[:, h * 128 : (h + 1) * 128]
        return jnp.concatenate(
            [
                thick.at[k, h][pl.ds(0, half_cols, stride=2), :]
                + thick.at[k, h][pl.ds(1, half_cols, stride=2), :]
                for h in range(parts)
            ],
            axis=1,
        )

    fetch_mass.wait()

    def gather_mass(y, carry):
        total = pairs(0, mass[2 * y] + mass[2 * y + 1])
        cscale[y + DEPTH, 8 : 8 + half_cols, :] = 0.8 / (4.0 + 0.5 * total)
        return carry

    lax.fori_loop(0, half_rows, gather_mass, 0, unroll=2)
    size = (half_rows, half_cols)
    send_scale = deep_copies(cscale, NEAR, size, coarse_send.at[0], coarse_recv.at[0])
    send_load = deep_copies(cload, NEAR, size, coarse_send.at[1], coarse_recv.at[1])
    send_value = deep_copies(coarse_c, DEPTH, size, coarse_send.at[2], coarse_recv.at[2])
    if SCALE_AT == 0:
        for copy in send_scale:
            copy.start()
    fetch_load.wait()

    def first(y, x0, x1, outer=True):
        here, total = fine.around(0, y, x0, x1, outer)
        weight = 0.8 / (4.0 + mass[y - 1, x0:x1, :])
        scale[y - 1, x0:x1, :] = weight
        fine.put(1, y, x0, x1, 0.2 * here + weight * (load[y - 1, x0:x1, :] + total), outer)

    fine.inside(first)
    fine.wait(0)
    fine.rim(0, first, fine.mend(0, scale))
    if SCALE_AT == 1:
        fine.start(1)
        for copy in send_scale:
            copy.start()
        fine.sweep(1, load, scale, begun=True)
    else:
        fine.sweep(1, load, scale)

    def defect(y, outer):
        here, total = fine.around(0, y, 0, cols, outer)
        return load[y - 1] + total - (4.0 + mass[y - 1]) * here

    def gather(y, outer):
        total = pairs(y % 2, defect(2 * y + 1, outer) + defect(2 * y + 2, outer))
        cload[y + DEPTH, 8 : 8 + half_cols, :] = 0.5 * total

    def gather_inner(y, carry):
        gather(y, False)
        return carry

    def gather_outer(y, carry):
        where = lax.broadcasted_iota(jnp.int32, (8, cases), 0)
        low = fine_got[0, 0, pl.ds(2 * y, 1), :] + fine_got[0, 0, pl.ds(2 * y + 1, 1), :]
        high = fine_got[0, 1, pl.ds(2 * y, 1), :] + fine_got[0, 1, pl.ds(2 * y + 1, 1), :]
        cload[y + DEPTH, 8:16, :] += jnp.where(where == 0, 0.5 * low, 0.0)
        cload[y + DEPTH, half_cols : half_cols + 8, :] += jnp.where(where == 7, 0.5 * high, 0.0)
        return carry

    fine.start(0)
    if SCALE_AT == 2:
        for copy in send_scale:
            copy.start()
    lax.fori_loop(1, half_rows - 1, gather_inner, 0, unroll=2)
    fine.wait(0)
    lax.fori_loop(1, half_rows - 1, gather_outer, 0, unroll=2)
    gather(0, True)
    gather(half_rows - 1, True)
    for end in (0, rows + 1):
        fine_b[end] = fine_a[end]
    for side in range(2):
        fine_got[1, side] = fine_got[0, side]
    for copy in send_load:
        copy.start()
    for copy in send_scale:
        copy.wait()
    for copy in send_load:
        copy.wait()

    tall, broad = cload.shape[0], cload.shape[1]

    def begin(y, carry):
        coarse_a[y] = cscale[y] * cload[y]
        return carry

    margin = DEPTH - NEAR
    lax.fori_loop(margin, tall - margin, begin, 0, unroll=2)

    def sweeps(chain, margin):
        for step, (old, new) in enumerate(zip(chain, chain[1:]), 1):
            own = new is coarse_c

            def row(y, carry, old=old, new=new, own=own):
                here = old[y]
                total = (pltpu.roll(here, 1, 0) + pltpu.roll(here, broad - 1, 0)) + (
                    old[y - 1] + old[y + 1]
                )
                value = 0.2 * here + cscale[y] * (cload[y] + total)
                if own:
                    new[y, 8 : 8 + half_cols, :] = value[8 : 8 + half_cols]
                else:
                    new[y] = value
                return carry

            lax.fori_loop(margin + step, tall - margin - step, row, 0, unroll=4)

    grids = (coarse_a, coarse_b)
    sweeps([grids[step % 2] for step in range(NEAR)] + [coarse_c], margin)
    for copy in send_value:
        copy.start()
    for copy in send_value:
        copy.wait()
    rest = INNER - 1 - NEAR
    sweeps([coarse_c] + [grids[step % 2] for step in range(rest)], 0)
    last = grids[(rest - 1) % 2]

    def widen(k, y):
        for h in range(parts):
            part = last[y, 8 : 8 + half_cols, h * 128 : (h + 1) * 128]
            spread.at[k, h][pl.ds(0, half_cols, stride=2), :] = part
            spread.at[k, h][pl.ds(1, half_cols, stride=2), :] = part
        return jnp.concatenate([spread[k, h] for h in range(parts)], axis=1)

    def correct(y, carry):
        added = widen(y % 2, y + DEPTH)
        low = last[y + DEPTH, 0:8, :][-1:]
        high = last[y + DEPTH, 8 + half_cols : 16 + half_cols, :][:1]
        for k in range(2):
            at = 2 * y + 1 + k
            fine_b[at] = fine_a[at] + added
            fine_got[1, 0, pl.ds(at - 1, 1), :] += low
            fine_got[1, 1, pl.ds(at - 1, 1), :] += high
        return carry

    lax.fori_loop(0, half_rows, correct, 0, unroll=2)
    fine_b[0] += widen(0, DEPTH - 1)
    fine_b[rows + 1] += widen(1, DEPTH + half_rows)
    fine.sweep(1, load, scale, own=True)
    fine.sweep(0, load, scale)

    def left(y, x0, x1, outer=True):
        here, total = fine.around(1, y, x0, x1, outer)
        fixed[y - 1, x0:x1, :] = here
        left_out[y - 1, x0:x1, :] = (
            load[y - 1, x0:x1, :] + total - (4.0 + mass[y - 1, x0:x1, :]) * here
        )

    fine.start(1)
    fine.inside(left)
    fine.wait(1)

    def mend_left(y, x0, x1, more):
        left_out[y - 1, x0:x1, :] += more

    fine.rim(1, left, mend_left)


def body(right_side, first_guess, mass_term):
    rows, cols, cases = right_side.shape
    half_rows, half_cols = rows // RATIO, cols // RATIO
    whole = jax.ShapeDtypeStruct(right_side.shape, jnp.float32)
    any_space = pl.BlockSpec(memory_space=pl.ANY)

    def vmem(*shape):
        return pltpu.VMEM(shape, jnp.float32)

    fixed, left = pl.pallas_call(
        kernel,
        out_shape=(pltpu.VMEM(right_side.shape, jnp.float32), pltpu.VMEM(right_side.shape, jnp.float32)),
        in_specs=[any_space] * 3,
        out_specs=(pl.BlockSpec(memory_space=pltpu.VMEM),)*2,
        scratch_shapes=[
            vmem(rows, cols, cases),
            vmem(rows, cols, cases),
            vmem(rows, cols, cases),
            vmem(rows + 2, cols, cases),
            vmem(rows + 2, cols, cases),
            vmem(2, 2, rows, cases),
            vmem(2, 2, rows, cases),
            vmem(2, cases // 128, cols, 128),
            vmem(half_rows + 2 * DEPTH, half_cols + 16, cases),
            vmem(half_rows + 2 * DEPTH, half_cols + 16, cases),
            vmem(half_rows + 2 * DEPTH, half_cols + 16, cases),
            vmem(half_rows + 2 * DEPTH, half_cols + 16, cases),
            vmem(half_rows + 2 * DEPTH, half_cols + 16, cases),
            vmem(2, cases // 128, cols, 128),
            pltpu.SemaphoreType.DMA((2, 4)),
            pltpu.SemaphoreType.DMA((2, 4)),
            pltpu.SemaphoreType.DMA((3, 8)),
            pltpu.SemaphoreType.DMA((3, 8)),
            pltpu.SemaphoreType.DMA((3,)),
        ],
        compiler_params=pltpu.CompilerParams(
            collective_id=0, has_side_effects=True, vmem_limit_bytes=48 * 1024 * 1024
        ),
    )(right_side, first_guess, mass_term)
    return fixed, left


def solution(mesh):
    spec = P("north", "east", None)
    return jax.shard_map(
        body, mesh=mesh, in_specs=(spec, spec, spec), out_specs=(spec, spec), check_vma=False
    )
```
